128 devices in a mesh: grp: 32 (over z, y, core), mem: 4 (over x).
Axes of the slice: x: 4, y: 4, z: 4, core: 2. Of those that a mesh axis runs over, the one named last changes fastest.
Arguments:
- tiles: bfloat16 [768, 11, 256, 256], P(('grp', 'mem')), as said below
- mask: int32 [768, 11], P(('grp', 'mem')), may hold values from 0 to 1, as said below
- branch: int32 [768], P(('grp', 'mem')), may hold values from 0 to 1
Outputs:
- new_tiles: float32 [768, 11, 256, 256], P(('grp', 'mem'))
- traces: float32 [2], replicated
The draws below stay inside these ranges and needn't reach their ends.
Inputs may be any that keep to these rules, and one draw needn't show every extreme that they name: X is symmetric: for |d| <= 5, wherever rows i and i + d both lie in the matrix, tiles[i + d, 5 - d] is exactly the transpose of tiles[i, 5 + d]. mask is symmetric in the same way (mask[i + d, 5 - d] == mask[i, 5 + d]); the diagonal slot mask[i, 5] is always 1; slots whose column i - 5 + s lies outside the matrix are 0.
All inputs are finite; a program needn't handle non-finite values.
Results may differ from the reference program's by a relative error of at most 0.0003.
Values may be sent and summed in bfloat16 or wider, within the bound.
No kernel may reach another device: no remote copies, remote signals or barrier semaphores. Data moves between devices by JAX's collectives and lax.ppermute only.
A program may use at most 256 MiB of HBM per device.

```python
import math
import jax
import jax.numpy as jnp
from jax import lax

TILE = 256
BAND = 5
ROWS_DEV = 6
SLOTS = 11
NTILES = 768
ORDER = 196608


def draw_tiles(key, part):
    subkeys = jax.random.split(key, 4)
    spread = 0.8 / math.sqrt(TILE)
    upper_draw = jax.random.normal(subkeys[0], (NTILES, BAND, TILE, TILE), jnp.float32)
    centre_draw = jax.random.normal(subkeys[1], (NTILES, TILE, TILE), jnp.float32)
    position = jnp.arange(ORDER, dtype=jnp.float32) / ORDER
    row_scale = (0.8 + 0.6 * position).reshape(NTILES, TILE)
    diagonal = jax.random.uniform(subkeys[3], (NTILES, TILE), jnp.float32, 0.2, 1.0)
    mirrored = (centre_draw + jnp.swapaxes(centre_draw, 1, 2)) * (0.5 * spread)
    mirrored = mirrored + jnp.eye(TILE, dtype=jnp.float32)[None] * diagonal[:, :, None]
    middle = mirrored * (row_scale[:, :, None] * row_scale[:, None, :])
    above_tiles = []
    for offset in range(1, BAND + 1):
        partner = jnp.roll(row_scale, -offset, axis=0)
        above_tiles.append(upper_draw[:, offset - 1] * spread * (row_scale[:, :, None] * partner[:, None, :]))
    below_tiles = [jnp.swapaxes(jnp.roll(above_tiles[offset - 1], offset, axis=0), 1, 2) for offset in range(BAND, 0, -1)]
    return jnp.stack(below_tiles + [middle] + above_tiles, axis=1).astype(jnp.bfloat16)


def draw_mask(key, part):
    subkeys = jax.random.split(key, 2)
    level_index = jax.random.randint(subkeys[0], (NTILES // ROWS_DEV,), 0, 4)
    level_table = jnp.array([20, 35, 50, 100], dtype=jnp.int32)
    row_levels = jnp.repeat(jnp.take(level_table, level_index), ROWS_DEV)
    coin_draw = jax.random.randint(subkeys[1], (NTILES, BAND), 0, 100)
    upper_mask = (coin_draw < row_levels[:, None]).astype(jnp.int32)
    indices = jnp.arange(NTILES, dtype=jnp.int32)
    columns = []
    for slot_index in range(SLOTS):
        offset = slot_index - BAND
        if offset == 0:
            columns.append(jnp.ones((NTILES,), jnp.int32))
        elif offset > 0:
            columns.append(upper_mask[:, offset - 1] * (indices + offset < NTILES).astype(jnp.int32))
        else:
            distance = -offset
            columns.append(jnp.roll(upper_mask[:, distance - 1], distance) * (indices - distance >= 0).astype(jnp.int32))
    return jnp.stack(columns, axis=1)


def place_ends(values, key, least, largest):
    shape = values.shape
    place = [jax.random.randint(jax.random.fold_in(key, axis), (), 0, shape[axis]) for axis in range(len(shape))]
    values = values.at[tuple(place)].set(least)
    longest = shape.index(max(shape))
    place[longest] = (place[longest] + 1) % shape[longest]
    return values.at[tuple(place)].set(largest)


def setup_inputs(seed: int = 0) -> dict:
    keys = jax.random.split(jax.random.key(seed), 4)
    tiles = draw_tiles(jax.random.fold_in(keys[3], 71), 0)
    mask = draw_mask(jax.random.fold_in(keys[3], 71), 0)
    branch = place_ends(jax.random.randint(keys[2], (NTILES,), 0, 2), jax.random.fold_in(keys[2], 1), 0, 1).astype(jnp.int32)
    return {"tiles": tiles, "mask": mask, "branch": branch}


def band_square(extended, row_count, half_band, slot_count):
    pieces = []
    for column in range(slot_count):
        first_slot = max(0, column - half_band)
        last_slot = min(slot_count - 1, column + half_band)
        left_tiles = extended[half_band:half_band + row_count, first_slot:last_slot + 1].astype(jnp.float32)
        right_tiles = jnp.stack([extended[through:through + row_count, column - through + half_band] for through in range(first_slot, last_slot + 1)], axis=1).astype(jnp.float32)
        pieces.append(jnp.einsum("rpab,rpbc->rac", left_tiles, right_tiles))
    return jnp.stack(pieces, axis=1)


def reference(tiles, mask, branch):
    occupied = mask[:, :, None, None]
    masked = tiles * occupied.astype(tiles.dtype)
    padded = jnp.pad(masked, ((BAND, BAND), (0, 0), (0, 0), (0, 0)))

    def square_block(first_row):
        window = lax.dynamic_slice_in_dim(padded, first_row, ROWS_DEV + 2 * BAND, 0)
        square = band_square(window, ROWS_DEV, BAND, SLOTS)
        own_rows = lax.dynamic_slice_in_dim(masked, first_row, ROWS_DEV, 0).astype(jnp.float32)
        keeper = lax.dynamic_slice_in_dim(occupied, first_row, ROWS_DEV, 0).astype(jnp.float32)
        selector = lax.dynamic_slice_in_dim(branch, first_row, ROWS_DEV, 0)[:, None, None, None]
        updated = jnp.where(selector == 0, square, 2.0 * own_rows - square) * keeper
        trace_part = jnp.sum(jnp.diagonal(updated[:, BAND], axis1=1, axis2=2))
        purity_part = jnp.sum(updated * updated)
        return updated, trace_part, purity_part

    starts = jnp.arange(NTILES // ROWS_DEV, dtype=jnp.int32) * ROWS_DEV
    updated, trace_parts, purity_parts = lax.map(square_block, starts)
    new_tiles = updated.reshape(NTILES, SLOTS, TILE, TILE)
    traces = jnp.stack([jnp.sum(trace_parts), jnp.sum(purity_parts)]) / ORDER
    return new_tiles, traces
```

```python
import jax
import jax.numpy as jnp
from jax import lax
from jax.experimental import pallas as pl
from jax.experimental.pallas import tpu as pltpu
from jax.sharding import Mesh
from jax.sharding import PartitionSpec as P

GRP_MEM = ("grp_0", "grp_1", "grp_2", "mem")
GRP = ("grp_0", "grp_1", "grp_2")
TILE = 256
HALF = 128
ROWS = 6
BAND = 5
SLOTS = 11
EXTRA = 16
MIB = 2**20

NEAR = ((1, 5), (2, 5), (3, 4), (3, 5), (4, 5), (3, 3), (4, 4), (5, 5))
FAR = ((1, 2), (1, 3), (1, 4), (2, 3), (2, 4), (1, 1), (2, 2))


def full_of(pairs):
    return [pair for pair in pairs if pair[0] != pair[1]]


def diag_of(pairs):
    return [pair for pair in pairs if pair[0] == pair[1]]


def chunk_rows(pairs):
    return TILE * len(full_of(pairs)) + HALF * len(diag_of(pairs)) + EXTRA


def shift(value, steps):
    count = lax.axis_size(GRP_MEM)
    first, last = max(0, -steps), min(count, count - steps)
    return lax.ppermute(value, GRP_MEM, [(source, source + steps) for source in range(first, last)])


def iotas(shape):
    return lax.broadcasted_iota(jnp.int32, shape, 0), lax.broadcasted_iota(jnp.int32, shape, 1)


def smem():
    return pl.BlockSpec(memory_space=pltpu.SMEM)


def vmem():
    return pl.BlockSpec(memory_space=pltpu.VMEM)


def hbm():
    return pl.BlockSpec(memory_space=pltpu.HBM)


def params(mib):
    return pltpu.CompilerParams(vmem_limit_bytes=mib * MIB)


def cost(products, tiles_moved):
    return pl.CostEstimate(
        flops=2 * TILE**3 * products, bytes_accessed=tiles_moved * TILE * TILE * 2, transcendentals=0
    )


def pack_corners(tiles, mask, branch, plan, name):
    diag_count = sum(len(diag_of(pairs)) for pairs, _ in plan)
    copy_count = sum(len(pairs) for pairs, _ in plan)

    def body(mask_ref, branch_ref, tiles_ref, *refs):
        outs, (diag_ref, sems) = refs[: len(plan)], refs[len(plan) :]
        copies = []
        diag = 0
        for (pairs, first_row), out in zip(plan, outs):
            for place, (p, q) in enumerate(full_of(pairs)):
                row, slot = p - 1 + first_row, q - p + BAND
                target = out.at[pl.ds(place * TILE, TILE)]
                copies.append((tiles_ref.at[row, slot], target))
            for p, _ in diag_of(pairs):
                copies.append((tiles_ref.at[p - 1 + first_row, BAND], diag_ref.at[diag]))
                diag += 1
        copies = [
            pltpu.make_async_copy(source, target, sems.at[number])
            for number, (source, target) in enumerate(copies)
        ]
        for copy in copies:
            copy.start()
        rows, columns = iotas((HALF, HALF))
        extra_rows, _ = iotas((EXTRA, TILE))
        number = 0
        diag = 0
        for (pairs, first_row), out in zip(plan, outs):
            for place, (p, q) in enumerate(full_of(pairs)):
                row, slot = p - 1 + first_row, q - p + BAND
                copies[number].wait()
                number += 1

                @pl.when(mask_ref[row, slot] == 0)
                def _(out=out, place=place):
                    out[pl.ds(place * TILE, TILE), :] = jnp.zeros((TILE, TILE), jnp.bfloat16)

            base = TILE * len(full_of(pairs))
            extra = jnp.zeros((EXTRA, TILE), jnp.float32)
            for place, (p, _) in enumerate(diag_of(pairs)):
                copies[number].wait()
                number += 1
                keep = mask_ref[p - 1 + first_row, BAND].astype(jnp.float32)
                tile = diag_ref[diag].astype(jnp.float32) * keep
                diag += 1
                low = tile[HALF:, HALF:]
                folded = jnp.where(columns <= rows, tile[:HALF, :HALF], low)
                at = pl.ds(base + place * HALF, HALF)
                out[at, pl.ds(0, HALF)] = tile[HALF:, :HALF].astype(jnp.bfloat16)
                out[at, pl.ds(HALF, HALF)] = folded.astype(jnp.bfloat16)
                line = jnp.sum(jnp.where(columns == rows, low, 0.0), axis=0, keepdims=True)
                line = jnp.concatenate([line, line], axis=1)
                extra = jnp.where(extra_rows == place, line, extra)
            for p in range(1, BAND + 1):
                flag = jnp.where(branch_ref[p - 1 + first_row] == 0, 0.0, 1.0)
                extra = jnp.where(extra_rows == 7 + p, flag, extra)
            out[pl.ds(base + HALF * len(diag_of(pairs)), EXTRA), :] = extra.astype(jnp.bfloat16)

    return pl.pallas_call(
        body,
        out_shape=[
            jax.ShapeDtypeStruct((chunk_rows(pairs), TILE), jnp.bfloat16) for pairs, _ in plan
        ],
        in_specs=[smem(), smem(), hbm()],
        out_specs=[vmem() for _ in plan],
        scratch_shapes=[
            pltpu.VMEM((diag_count, TILE, TILE), jnp.bfloat16),
            pltpu.SemaphoreType.DMA((copy_count,)),
        ],
        compiler_params=params(16),
        cost_estimate=cost(1, 4 * copy_count),
        name=name,
    )(mask, branch, tiles)


class Corner:
    def __init__(self, square_ref):
        self.square_ref = square_ref
        self.where = {}
        self.count = 0

    def add(self, chunk, pairs):
        rows, columns = iotas((HALF, HALF))
        for place, pair in enumerate(full_of(pairs)):
            self.where[pair] = (chunk, pl.ds(place * TILE, TILE))
        base = TILE * len(full_of(pairs))
        extra = chunk[pl.ds(base + HALF * len(diag_of(pairs)), EXTRA), :].astype(jnp.float32)
        for place, pair in enumerate(diag_of(pairs)):
            at = pl.ds(base + place * HALF, HALF)
            corner = chunk[at, pl.ds(0, HALF)].astype(jnp.float32)
            folded = chunk[at, pl.ds(HALF, HALF)].astype(jnp.float32)
            turned = folded.T
            line = extra[place : place + 1, :HALF]
            high = jnp.where(columns <= rows, folded, turned)
            low = jnp.where(columns > rows, folded, turned)
            low = jnp.where(columns == rows, line, low)
            target = self.square_ref.at[self.count]
            target[pl.ds(0, HALF), pl.ds(0, HALF)] = high.astype(jnp.bfloat16)
            target[pl.ds(HALF, HALF), pl.ds(HALF, HALF)] = low.astype(jnp.bfloat16)
            target[pl.ds(HALF, HALF), pl.ds(0, HALF)] = corner.astype(jnp.bfloat16)
            target[pl.ds(0, HALF), pl.ds(HALF, HALF)] = corner.T.astype(jnp.bfloat16)
            self.where[pair] = (target, slice(None))
            self.count += 1
        return extra

    def times(self, left, p, q):
        chunk, at = self.where[(min(p, q), max(p, q))]
        return dot(left, chunk[at, :], p > q)


def dot(left, right, transposed):
    return lax.dot_general(
        left, right, (((1,), (1 if transposed else 0,)), ((), ())), preferred_element_type=jnp.float32
    )


def polynomial(square, own, keep, bent):
    return (keep * (1.0 - 2.0 * bent)) * square + (keep * (2.0 * bent)) * own


def squares(value):
    return jnp.sum((value * value).reshape(TILE // 8, 8, TILE), axis=0)


def scalars(mask_ref, branch_ref, row, slot):
    keep = mask_ref[row, slot].astype(jnp.float32)
    bent = jnp.where(branch_ref[row] == 0, 0.0, 1.0)
    return keep, bent


def inner_tiles(tiles, mask, branch, after):
    inner = [(i, j) for i in range(ROWS) for j in range(ROWS)]

    def body(mask_ref, branch_ref, tiles_ref, _, out_ref, sums_ref, own_ref, new_ref, in_sems, out_sems):
        loads = [
            pltpu.make_async_copy(tiles_ref.at[row], own_ref.at[row], in_sems.at[row])
            for row in range(ROWS)
        ]
        for load in loads:
            load.start()
        for row, load in enumerate(loads):
            load.wait()
            for slot in range(SLOTS):

                @pl.when(mask_ref[row, slot] == 0)
                def _(row=row, slot=slot):
                    own_ref[row, slot] = jnp.zeros((TILE, TILE), jnp.bfloat16)

        rows, columns = iotas((TILE, TILE))
        total = jnp.zeros((8, TILE), jnp.float32)
        trace = jnp.zeros((8, TILE), jnp.float32)
        stores = []

        def emit(i, j, square):
            slot = j - i + BAND
            keep, bent = scalars(mask_ref, branch_ref, i, slot)
            value = polynomial(square, own_ref[i, slot].astype(jnp.float32), keep, bent)
            number = i * ROWS + j
            new_ref[number] = value
            stores.append(
                pltpu.make_async_copy(new_ref.at[number], out_ref.at[i, slot], out_sems.at[number])
            )
            stores[-1].start()
            return value

        for i in range(ROWS):
            for j in range(i, ROWS):
                square = None
                for k in range(j - BAND, i + BAND + 1):
                    left = own_ref[i, k - i + BAND]
                    if 0 <= k < ROWS:
                        term = dot(left, own_ref[k, j - k + BAND], False)
                    else:
                        term = dot(left, own_ref[j, k - j + BAND], True)
                    square = term if square is None else square + term
                value = emit(i, j, square)
                total = total + squares(value)
                if i == j:
                    part = jnp.where(rows == columns, value, 0.0)
                    trace = trace + jnp.sum(part.reshape(TILE // 8, 8, TILE), axis=0)
                else:
                    total = total + squares(emit(j, i, square.T))
        sums_ref[pl.ds(0, 8), :] = total
        sums_ref[pl.ds(8, 8), :] = trace
        for store in stores:
            store.wait()

    return pl.pallas_call(
        body,
        out_shape=[
            jax.ShapeDtypeStruct((ROWS, SLOTS, TILE, TILE), jnp.float32),
            jax.ShapeDtypeStruct((16, TILE), jnp.float32),
        ],
        in_specs=[smem(), smem(), hbm(), hbm()],
        out_specs=[hbm(), vmem()],
        scratch_shapes=[
            pltpu.VMEM((ROWS, SLOTS, TILE, TILE), jnp.bfloat16),
            pltpu.VMEM((len(inner), TILE, TILE), jnp.float32),
            pltpu.SemaphoreType.DMA((ROWS,)),
            pltpu.SemaphoreType.DMA((len(inner),)),
        ],
        compiler_params=params(32),
        cost_estimate=cost(196, 66 + 72),
        name="inner",
    )(mask, branch, tiles, after)


def cross_tiles(tiles, mask, branch, made, above, below, up_pairs, down_pairs, sums, name):
    outputs = []
    for r, q in up_pairs:
        i, j = r - 1, q - 6
        terms = [((i, k - i + BAND), ("own", k, j - k + BAND)) for k in range(q)]
        terms += [((i, p - 6 - i + BAND), ("above", p, q)) for p in range(r, BAND + 1)]
        outputs.append((i, j - i + BAND, terms, ("above", q)))
    for r, q in down_pairs:
        i, j = q, 5 + r
        terms = [((i, k - i + BAND), ("own", k, j - k + BAND)) for k in range(r, ROWS)]
        terms += [((i, 5 + p - i + BAND), ("below", p, r)) for p in range(1, q + 1)]
        outputs.append((i, j - i + BAND, terms, ("below", r)))
    needed = []
    for i, slot, terms, _ in outputs:
        for left, right in terms:
            needed += [left] + ([right[1:]] if right[0] == "own" else [])
        needed.append((i, slot))
    needed = list(dict.fromkeys(needed))
    place = {key: number for number, key in enumerate(needed)}
    chunks = [("above", pairs, chunk) for pairs, chunk in above]
    chunks += [("below", pairs, chunk) for pairs, chunk in below]
    diag_count = {
        side: sum(len(diag_of(pairs)) for which, pairs, _ in chunks if which == side)
        for side in ("above", "below")
    }
    reduce = sums is not None
    group = 1
    if reduce:
        for axis in GRP:
            group *= lax.axis_size(axis)

    def body(mask_ref, branch_ref, tiles_ref, _, *refs):
        refs = list(refs)
        landed = [refs.pop(0) for _ in chunks]
        sums_ref = refs.pop(0) if reduce else None
        out_ref = refs.pop(0)
        red_ref = refs.pop(0) if reduce else None
        own_ref, above_ref, below_ref, new_ref, in_sems, out_sems = refs
        loads = [
            pltpu.make_async_copy(tiles_ref.at[row, slot], own_ref.at[number], in_sems.at[number])
            for number, (row, slot) in enumerate(needed)
        ]
        for load in loads:
            load.start()
        corners = {"above": Corner(above_ref), "below": Corner(below_ref)}
        flags = {}
        for (side, pairs, _), chunk_ref in zip(chunks, landed):
            flags.setdefault(side, corners[side].add(chunk_ref, pairs))
        ready = set()

        def own(row, slot):
            number = place[(row, slot)]
            if number not in ready:
                ready.add(number)
                loads[number].wait()
                keep = mask_ref[row, slot].astype(jnp.float32).astype(jnp.bfloat16)
                own_ref[number] = own_ref[number] * keep
            return own_ref[number]

        total = jnp.zeros((8, TILE), jnp.float32)
        stores = []
        for number, (i, slot, terms, (side, other)) in enumerate(outputs):
            square = None
            for left, right in terms:
                if right[0] == "own":
                    term = dot(own(*left), own(*right[1:]), False)
                else:
                    term = corners[right[0]].times(own(*left), *right[1:])
                square = term if square is None else square + term
            keep, bent = scalars(mask_ref, branch_ref, i, slot)
            mine = own(i, slot).astype(jnp.float32)
            value = polynomial(square, mine, keep, bent)
            new_ref[number] = value
            stores.append(
                pltpu.make_async_copy(new_ref.at[number], out_ref.at[i, slot], out_sems.at[number])
            )
            stores[-1].start()
            if reduce:
                bent = flags[side][7 + other : 8 + other, :]
                mirror = polynomial(square, mine, keep, bent)
                total = total + squares(value) + squares(mirror)
        if reduce:
            purity = jnp.sum(total + sums_ref[pl.ds(0, 8), :], keepdims=True)
            trace = jnp.sum(sums_ref[pl.ds(8, 8), :], keepdims=True)
            _, lanes = iotas((group, HALF))
            red_ref[...] = jnp.where(lanes == 0, trace, jnp.where(lanes == 1, purity, 0.0))
        for store in stores:
            store.wait()

    products = sum(len(terms) for _, _, terms, _ in outputs)
    out_shape = [jax.ShapeDtypeStruct(made.shape, made.dtype)]
    out_specs = [hbm()]
    if reduce:
        out_shape.append(jax.ShapeDtypeStruct((group, HALF), jnp.float32))
        out_specs.append(vmem())
    return pl.pallas_call(
        body,
        out_shape=out_shape,
        in_specs=[smem(), smem(), hbm(), hbm()] + [vmem() for _ in chunks] + [vmem()] * reduce,
        out_specs=out_specs,
        scratch_shapes=[
            pltpu.VMEM((len(needed), TILE, TILE), jnp.bfloat16),
            pltpu.VMEM((diag_count["above"], TILE, TILE), jnp.bfloat16),
            pltpu.VMEM((diag_count["below"], TILE, TILE), jnp.bfloat16),
            pltpu.VMEM((len(outputs), TILE, TILE), jnp.float32),
            pltpu.SemaphoreType.DMA((len(needed),)),
            pltpu.SemaphoreType.DMA((len(outputs),)),
        ],
        input_output_aliases={3: 0},
        compiler_params=params(32),
        cost_estimate=cost(products, 66 + 2 * len(outputs)),
        name=name,
    )(mask, branch, tiles, made, *[chunk for _, _, chunk in chunks], *([sums] if reduce else []))


def on_device(tiles, mask, branch):
    tiles, mask, branch = (
        pltpu.with_memory_space_constraint(value, pltpu.HBM) for value in (tiles, mask, branch)
    )
    down_first, up_first = pack_corners(tiles, mask, branch, ((NEAR, 1), (FAR, 0)), "pack_first")
    above_first, below_first = shift(down_first, 1), shift(up_first, -1)
    down_last, up_last = pack_corners(tiles, mask, branch, ((FAR, 1), (NEAR, 0)), "pack_last")
    above_last, below_last = shift(down_last, 1), shift(up_last, -1)
    made, sums = inner_tiles(tiles, mask, branch, up_last)
    made, part = cross_tiles(
        tiles, mask, branch, made, [(NEAR, above_first)], [(FAR, below_first)], NEAR, FAR, sums, "cross_first"
    )
    parts = lax.all_to_all(part, GRP, 0, 0, tiled=True)
    part = jnp.sum(parts, axis=0, keepdims=True)

    def partner(bits):
        return lax.ppermute(part, "mem", [(m, m ^ bits) for m in range(lax.axis_size("mem"))])

    others = [partner(bits) for bits in (1, 2, 3)]
    part, made = lax.optimization_barrier((part, made))
    (made,) = cross_tiles(
        tiles,
        mask,
        branch,
        made,
        [(NEAR, above_first), (FAR, above_last)],
        [(FAR, below_first), (NEAR, below_last)],
        FAR,
        NEAR,
        None,
        "cross_last",
    )
    traces = (part + others[0]) + (others[1] + others[2])
    order = ROWS * lax.axis_size(GRP_MEM) * TILE
    return made, traces[0, :2] / order


def solution(mesh):
    torus = Mesh(
        mesh.devices.reshape(4, 4, 2, mesh.shape["mem"]), ("grp_0", "grp_1", "grp_2", "mem")
    )
    placed = (P(GRP_MEM, None, None, None), P(GRP_MEM, None), P(GRP_MEM))
    return jax.shard_map(
        on_device,
        mesh=torus,
        in_specs=placed,
        out_specs=(P(GRP_MEM, None, None, None), P()),
        check_vma=False,
    )
```

```python
import jax
import jax.numpy as jnp
from jax import lax
from jax.experimental import pallas as pl
from jax.experimental.pallas import tpu as pltpu
from jax.sharding import Mesh
from jax.sharding import PartitionSpec as P

GRP_MEM = ("grp_0", "grp_1", "grp_2", "mem")
GRP = ("grp_0", "grp_1", "grp_2")
TILE = 256
HALF = 128
ROWS = 6
BAND = 5
SLOTS = 11
EXTRA = 16
PREFETCH = 600
MIB = 2**20

NEAR = ((1, 5), (2, 5), (3, 4), (3, 5), (4, 5), (3, 3), (4, 4), (5, 5))
FAR = ((1, 2), (1, 3), (1, 4), (2, 3), (2, 4), (1, 1), (2, 2))


def full_of(pairs):
    return [pair for pair in pairs if pair[0] != pair[1]]


def diag_of(pairs):
    return [pair for pair in pairs if pair[0] == pair[1]]


def chunk_rows(pairs):
    return TILE * len(full_of(pairs)) + HALF * len(diag_of(pairs)) + EXTRA


def shift(value, steps):
    count = lax.axis_size(GRP_MEM)
    first, last = max(0, -steps), min(count, count - steps)
    return lax.ppermute(value, GRP_MEM, [(source, source + steps) for source in range(first, last)])


def iotas(shape):
    return lax.broadcasted_iota(jnp.int32, shape, 0), lax.broadcasted_iota(jnp.int32, shape, 1)


def smem():
    return pl.BlockSpec(memory_space=pltpu.SMEM)


def vmem():
    return pl.BlockSpec(memory_space=pltpu.VMEM)


def hbm():
    return pl.BlockSpec(memory_space=pltpu.HBM)


def params(mib):
    return pltpu.CompilerParams(vmem_limit_bytes=mib * MIB)


def cost(products, tiles_moved):
    return pl.CostEstimate(
        flops=2 * TILE**3 * products, bytes_accessed=tiles_moved * TILE * TILE * 2, transcendentals=0
    )


def write_chunk(out, base, pairs, first_row, branch_ref, diag_tile):
    rows, columns = iotas((HALF, HALF))
    extra_rows, _ = iotas((EXTRA, TILE))
    extra = jnp.zeros((EXTRA, TILE), jnp.float32)
    for place, (p, _) in enumerate(diag_of(pairs)):
        tile = diag_tile(p - 1 + first_row)
        low = tile[HALF:, HALF:]
        folded = jnp.where(columns <= rows, tile[:HALF, :HALF], low)
        at = pl.ds(base + place * HALF, HALF)
        out[at, pl.ds(0, HALF)] = tile[HALF:, :HALF].astype(jnp.bfloat16)
        out[at, pl.ds(HALF, HALF)] = folded.astype(jnp.bfloat16)
        line = jnp.sum(jnp.where(columns == rows, low, 0.0), axis=0, keepdims=True)
        line = jnp.concatenate([line, line], axis=1)
        extra = jnp.where(extra_rows == place, line, extra)
    for p in range(1, BAND + 1):
        flag = jnp.where(branch_ref[p - 1 + first_row] == 0, 0.0, 1.0)
        extra = jnp.where(extra_rows == 7 + p, flag, extra)
    out[pl.ds(base + HALF * len(diag_of(pairs)), EXTRA), :] = extra.astype(jnp.bfloat16)


def local_copies(pairs_of_refs, sems):
    copies = [
        pltpu.make_async_copy(source, target, sems.at[number])
        for number, (source, target) in enumerate(pairs_of_refs)
    ]
    for copy in copies:
        copy.start()
    return copies


def pack_corners(tiles, mask, branch, first, last):
    plan = first + last
    diags = [(side, p) for side, (pairs, _) in enumerate(plan) for p, _ in diag_of(pairs)]
    fulls = [(side, place, p, q) for side, (pairs, _) in enumerate(plan) for place, (p, q) in enumerate(full_of(pairs))]
    early = [full for full in fulls if full[0] < len(first)]
    late = [full for full in fulls if full[0] >= len(first)]

    def tail_rows(pairs):
        return HALF * len(diag_of(pairs)) + EXTRA

    def body(mask_hbm, branch_hbm, tiles_ref, *refs):
        outs, refs = refs[: len(plan)], refs[len(plan) :]
        tails, refs = refs[: len(last)], refs[len(last) :]
        mask_ref, branch_ref, diag_ref, zero_ref, table_sems, early_sems, diag_sems, late_sems, tail_sems = refs

        def spot(side, p, q):
            return p - 1 + plan[side][1], q - p + BAND

        tables = local_copies([(mask_hbm, mask_ref), (branch_hbm, branch_ref)], table_sems)
        early_copies = local_copies(
            [
                (tiles_ref.at[spot(side, p, q)], outs[side].at[pl.ds(place * TILE, TILE)])
                for side, place, p, q in early
            ],
            early_sems,
        )
        diag_copies = local_copies(
            [(tiles_ref.at[spot(side, p, p)], diag_ref.at[number]) for number, (side, p) in enumerate(diags)],
            diag_sems,
        )
        zero_ref[...] = jnp.zeros((TILE, TILE), jnp.bfloat16)
        for table in tables:
            table.wait()
        late_copies = []
        for number, (side, place, p, q) in enumerate(late):
            target = outs[side].at[pl.ds(place * TILE, TILE)]
            copy = pltpu.make_async_copy(tiles_ref.at[spot(side, p, q)], target, late_sems.at[number])
            blank = pltpu.make_async_copy(zero_ref, target, late_sems.at[number])
            occupied = mask_ref[spot(side, p, q)] != 0
            pl.when(occupied)(copy.start)
            pl.when(jnp.logical_not(occupied))(blank.start)
            late_copies.append(copy)
        for copy, (side, place, p, q) in zip(early_copies, early):
            copy.wait()

            @pl.when(mask_ref[spot(side, p, q)] == 0)
            def _(out=outs[side], place=place):
                out[pl.ds(place * TILE, TILE), :] = jnp.zeros((TILE, TILE), jnp.bfloat16)

        for copy in diag_copies:
            copy.wait()
        tail_copies = []
        for side, (pairs, first_row) in enumerate(plan):

            def diag_tile(row, side=side, first_row=first_row):
                number = diags.index((side, row + 1 - first_row))
                return diag_ref[number].astype(jnp.float32) * mask_ref[row, BAND].astype(jnp.float32)

            base = TILE * len(full_of(pairs))
            if side < len(first):
                write_chunk(outs[side], base, pairs, first_row, branch_ref, diag_tile)
            else:
                tail = tails[side - len(first)]
                write_chunk(tail, 0, pairs, first_row, branch_ref, diag_tile)
                target = outs[side].at[pl.ds(base, tail_rows(pairs))]
                tail_copies.append(pltpu.make_async_copy(tail, target, tail_sems.at[side - len(first)]))
                tail_copies[-1].start()
        for copy in late_copies + tail_copies:
            copy.wait()

    return pl.pallas_call(
        body,
        out_shape=[
            jax.ShapeDtypeStruct((chunk_rows(pairs), TILE), jnp.bfloat16) for pairs, _ in plan
        ],
        in_specs=[hbm(), hbm(), hbm()],
        out_specs=[vmem() for _ in first] + [hbm() for _ in last],
        scratch_shapes=[pltpu.VMEM((tail_rows(pairs), TILE), jnp.bfloat16) for pairs, _ in last]
        + [
            pltpu.SMEM(mask.shape, mask.dtype),
            pltpu.SMEM(branch.shape, branch.dtype),
            pltpu.VMEM((len(diags), TILE, TILE), jnp.bfloat16),
            pltpu.VMEM((TILE, TILE), jnp.bfloat16),
            pltpu.SemaphoreType.DMA((2,)),
            pltpu.SemaphoreType.DMA((len(early),)),
            pltpu.SemaphoreType.DMA((len(diags),)),
            pltpu.SemaphoreType.DMA((len(late),)),
            pltpu.SemaphoreType.DMA((len(last),)),
        ],
        compiler_params=params(16),
        cost_estimate=cost(PREFETCH, PREFETCH),
        name="pack",
    )(mask, branch, tiles)


def half_scalar(value):
    return value.astype(jnp.float32).astype(jnp.bfloat16)


class Corner:
    def __init__(self, square_ref):
        self.square_ref = square_ref
        self.where = {}
        self.count = 0

    def add(self, chunk, pairs):
        rows, columns = iotas((HALF, HALF))
        for place, pair in enumerate(full_of(pairs)):
            self.where[pair] = (chunk, pl.ds(place * TILE, TILE))
        base = TILE * len(full_of(pairs))
        extra = chunk[pl.ds(base + HALF * len(diag_of(pairs)), EXTRA), :].astype(jnp.float32)
        for place, pair in enumerate(diag_of(pairs)):
            at = pl.ds(base + place * HALF, HALF)
            corner = chunk[at, pl.ds(0, HALF)].astype(jnp.float32)
            folded = chunk[at, pl.ds(HALF, HALF)].astype(jnp.float32)
            turned = folded.T
            line = extra[place : place + 1, :HALF]
            high = jnp.where(columns <= rows, folded, turned)
            low = jnp.where(columns > rows, folded, turned)
            low = jnp.where(columns == rows, line, low)
            target = self.square_ref.at[self.count]
            target[pl.ds(0, HALF), pl.ds(0, HALF)] = high.astype(jnp.bfloat16)
            target[pl.ds(HALF, HALF), pl.ds(HALF, HALF)] = low.astype(jnp.bfloat16)
            target[pl.ds(HALF, HALF), pl.ds(0, HALF)] = corner.astype(jnp.bfloat16)
            target[pl.ds(0, HALF), pl.ds(HALF, HALF)] = corner.T.astype(jnp.bfloat16)
            self.where[pair] = (target, slice(None))
            self.count += 1
        return extra

    def times(self, left, p, q):
        chunk, at = self.where[(min(p, q), max(p, q))]
        return dot(left, chunk[at, :], p > q)


def dot(left, right, transposed):
    return lax.dot_general(
        left, right, (((1,), (1 if transposed else 0,)), ((), ())), preferred_element_type=jnp.float32
    )


def polynomial(square, own, keep, bent):
    return (keep * (1.0 - 2.0 * bent)) * square + (keep * (2.0 * bent)) * own


def squares(value):
    return jnp.sum((value * value).reshape(TILE // 8, 8, TILE), axis=0)


def scalars(mask_ref, branch_ref, row, slot):
    keep = mask_ref[row, slot].astype(jnp.float32)
    bent = jnp.where(branch_ref[row] == 0, 0.0, 1.0)
    return keep, bent


def cross_outputs(up_pairs, down_pairs):
    outputs = []
    for r, q in up_pairs:
        i, j = r - 1, q - 6
        near = [((i, k - i + BAND), (k, j - k + BAND)) for k in range(q)]
        far = [((i, p - 6 - i + BAND), (p, q)) for p in range(r, BAND + 1)]
        outputs.append((i, j - i + BAND, near, far, ("above", q)))
    for r, q in down_pairs:
        i, j = q, 5 + r
        near = [((i, k - i + BAND), (k, j - k + BAND)) for k in range(r, ROWS)]
        far = [((i, 5 + p - i + BAND), (p, r)) for p in range(1, q + 1)]
        outputs.append((i, j - i + BAND, near, far, ("below", r)))
    return outputs


def near_part(tiles_ref, mask_ref, near):
    square = None
    for left, right in near:
        scale = half_scalar(mask_ref[left] * mask_ref[right])
        term = dot(tiles_ref[left] * scale, tiles_ref[right], False)
        square = term if square is None else square + term
    return square


def inner_tiles(tiles, mask, branch, outputs):
    inner = [(i, j) for i in range(ROWS) for j in range(ROWS)]

    def body(mask_ref, branch_ref, tiles_ref, out_ref, sums_ref, parts_ref, new_ref, out_sems):
        rows, columns = iotas((TILE, TILE))
        total = jnp.zeros((8, TILE), jnp.float32)
        trace = jnp.zeros((8, TILE), jnp.float32)
        stores = []

        def emit(i, j, square):
            slot = j - i + BAND
            keep, bent = scalars(mask_ref, branch_ref, i, slot)
            value = polynomial(square, tiles_ref[i, slot].astype(jnp.float32), keep, bent)
            number = i * ROWS + j
            new_ref[number] = value
            stores.append(
                pltpu.make_async_copy(new_ref.at[number], out_ref.at[i, slot], out_sems.at[number])
            )
            stores[-1].start()
            return value

        for i in range(ROWS):
            for j in range(i, ROWS):
                square = None
                for k in range(j - BAND, i + BAND + 1):
                    left, down = (i, k - i + BAND), 0 <= k < ROWS
                    right = (k, j - k + BAND) if down else (j, k - j + BAND)
                    scale = half_scalar(mask_ref[left] * mask_ref[right])
                    term = dot(tiles_ref[left] * scale, tiles_ref[right], not down)
                    square = term if square is None else square + term
                value = emit(i, j, square)
                total = total + squares(value)
                if i == j:
                    part = jnp.where(rows == columns, value, 0.0)
                    trace = trace + jnp.sum(part.reshape(TILE // 8, 8, TILE), axis=0)
                else:
                    total = total + squares(emit(j, i, square.T))
        sums_ref[pl.ds(0, 8), :] = total
        sums_ref[pl.ds(8, 8), :] = trace
        for number, (_, _, near, _, _) in enumerate(outputs):
            parts_ref[number] = near_part(tiles_ref, mask_ref, near)
        for store in stores:
            store.wait()

    products = 196 + sum(len(output[2]) for output in outputs)
    return pl.pallas_call(
        body,
        out_shape=[
            jax.ShapeDtypeStruct((ROWS, SLOTS, TILE, TILE), jnp.float32),
            jax.ShapeDtypeStruct((16, TILE), jnp.float32),
            jax.ShapeDtypeStruct((len(outputs), TILE, TILE), jnp.float32),
        ],
        in_specs=[smem(), smem(), vmem()],
        out_specs=[hbm(), vmem(), vmem()],
        scratch_shapes=[
            pltpu.VMEM((len(inner), TILE, TILE), jnp.float32),
            pltpu.SemaphoreType.DMA((len(inner),)),
        ],
        compiler_params=params(24),
        cost_estimate=cost(products, 66 + 72),
        name="inner",
    )(mask, branch, tiles)


def cross_first(tiles, mask, branch, made, above, below, outputs, parts, sums):
    group = 1
    for axis in GRP:
        group *= lax.axis_size(axis)

    def body(
        mask_ref, branch_ref, tiles_ref, _, above_ref, below_ref, parts_ref, sums_ref,
        out_ref, red_ref, above_square, below_square, new_ref, out_sems,
    ):
        corners = {"above": Corner(above_square), "below": Corner(below_square)}
        flags = {"above": corners["above"].add(above_ref, NEAR), "below": corners["below"].add(below_ref, FAR)}
        total = jnp.zeros((8, TILE), jnp.float32)
        stores = []
        for number, (i, slot, _, far, (side, other)) in enumerate(outputs):
            square = None
            for left, right in far:
                term = corners[side].times(tiles_ref[left] * half_scalar(mask_ref[left]), *right)
                square = term if square is None else square + term
            square = square + parts_ref[number]
            keep, bent = scalars(mask_ref, branch_ref, i, slot)
            mine = tiles_ref[i, slot].astype(jnp.float32)
            value = polynomial(square, mine, keep, bent)
            new_ref[number] = value
            stores.append(
                pltpu.make_async_copy(new_ref.at[number], out_ref.at[i, slot], out_sems.at[number])
            )
            stores[-1].start()
            mirror = polynomial(square, mine, keep, flags[side][7 + other : 8 + other, :])
            total = total + squares(value) + squares(mirror)
        purity = jnp.sum(total + sums_ref[pl.ds(0, 8), :], keepdims=True)
        trace = jnp.sum(sums_ref[pl.ds(8, 8), :], keepdims=True)
        _, lanes = iotas((group, HALF))
        red_ref[...] = jnp.where(lanes == 0, trace, jnp.where(lanes == 1, purity, 0.0))
        for store in stores:
            store.wait()

    return pl.pallas_call(
        body,
        out_shape=[
            jax.ShapeDtypeStruct(made.shape, made.dtype),
            jax.ShapeDtypeStruct((group, HALF), jnp.float32),
        ],
        in_specs=[smem(), smem(), vmem(), hbm(), vmem(), vmem(), vmem(), vmem()],
        out_specs=[hbm(), vmem()],
        scratch_shapes=[
            pltpu.VMEM((len(diag_of(NEAR)), TILE, TILE), jnp.bfloat16),
            pltpu.VMEM((len(diag_of(FAR)), TILE, TILE), jnp.bfloat16),
            pltpu.VMEM((len(outputs), TILE, TILE), jnp.float32),
            pltpu.SemaphoreType.DMA((len(outputs),)),
        ],
        input_output_aliases={3: 0},
        compiler_params=params(16),
        cost_estimate=cost(sum(len(output[3]) for output in outputs), 66 + 2 * len(outputs)),
        name="cross_first",
    )(mask, branch, tiles, made, above, below, parts, sums)


def cross_last(tiles, mask, branch, made, above, below, outputs):
    def body(mask_ref, branch_ref, tiles_ref, _, *refs):
        chunk_refs, (out_ref, above_square, below_square, new_ref, out_sems) = refs[:4], refs[4:]
        corners = {"above": Corner(above_square), "below": Corner(below_square)}
        corners["above"].add(chunk_refs[0], NEAR)
        corners["above"].add(chunk_refs[1], FAR)
        corners["below"].add(chunk_refs[2], FAR)
        corners["below"].add(chunk_refs[3], NEAR)
        stores = []
        for number, output in enumerate(outputs):
            i, slot, near, far, (side, _) = output
            square = near_part(tiles_ref, mask_ref, near)
            for left, right in far:
                square = square + corners[side].times(tiles_ref[left] * half_scalar(mask_ref[left]), *right)
            keep, bent = scalars(mask_ref, branch_ref, i, slot)
            new_ref[number] = polynomial(square, tiles_ref[i, slot].astype(jnp.float32), keep, bent)
            stores.append(
                pltpu.make_async_copy(new_ref.at[number], out_ref.at[i, slot], out_sems.at[number])
            )
            stores[-1].start()
        for store in stores:
            store.wait()

    products = sum(len(output[2]) + len(output[3]) for output in outputs)
    return pl.pallas_call(
        body,
        out_shape=jax.ShapeDtypeStruct(made.shape, made.dtype),
        in_specs=[smem(), smem(), vmem(), hbm()] + [vmem() for _ in range(4)],
        out_specs=hbm(),
        scratch_shapes=[
            pltpu.VMEM((BAND, TILE, TILE), jnp.bfloat16),
            pltpu.VMEM((BAND, TILE, TILE), jnp.bfloat16),
            pltpu.VMEM((len(outputs), TILE, TILE), jnp.float32),
            pltpu.SemaphoreType.DMA((len(outputs),)),
        ],
        input_output_aliases={3: 0},
        compiler_params=params(16),
        cost_estimate=cost(products, 66 + 2 * len(outputs)),
        name="cross_last",
    )(mask, branch, tiles, made, *above, *below)


def add_rows(parts):
    def body(parts_ref, out_ref):
        out_ref[...] = jnp.sum(parts_ref[...], axis=0, keepdims=True)

    return pl.pallas_call(
        body,
        out_shape=jax.ShapeDtypeStruct((1, parts.shape[1]), parts.dtype),
        in_specs=[vmem()],
        out_specs=vmem(),
        compiler_params=params(4),
        cost_estimate=cost(PREFETCH, PREFETCH),
        name="add_rows",
    )(parts)


def on_device(tiles, mask, branch):
    held, mask, branch = (
        pltpu.with_memory_space_constraint(value, pltpu.HBM) for value in (tiles, mask, branch)
    )
    down_first, up_first, down_last, up_last = pack_corners(
        held, mask, branch, ((NEAR, 1), (FAR, 0)), ((FAR, 1), (NEAR, 0))
    )
    above_first, below_first = shift(down_first, 1), shift(up_first, -1)
    above_last = shift(down_last, 1)
    below_last = shift(up_last, -1)
    outputs = cross_outputs(NEAR, FAR)
    made, sums, parts = inner_tiles(tiles, mask, branch, outputs)
    made, part = cross_first(
        tiles, mask, branch, made, above_first, below_first, outputs, parts, sums
    )
    part = add_rows(lax.all_to_all(part, GRP, 0, 0, tiled=True))

    def partner(bits):
        return lax.ppermute(part, "mem", [(m, m ^ bits) for m in range(lax.axis_size("mem"))])

    others = [partner(bits) for bits in (1, 2, 3)]
    part, made = lax.optimization_barrier((part, made))
    made = cross_last(
        tiles,
        mask,
        branch,
        made,
        (above_first, above_last),
        (below_first, below_last),
        cross_outputs(FAR, NEAR),
    )
    traces = (part + others[0]) + (others[1] + others[2])
    order = ROWS * lax.axis_size(GRP_MEM) * TILE
    return made, traces[0, :2] / order


def solution(mesh):
    torus = Mesh(
        mesh.devices.reshape(4, 4, 2, mesh.shape["mem"]), ("grp_0", "grp_1", "grp_2", "mem")
    )
    placed = (P(GRP_MEM, None, None, None), P(GRP_MEM, None), P(GRP_MEM))

    return jax.shard_map(
        on_device,
        mesh=torus,
        in_specs=placed,
        out_specs=(P(GRP_MEM, None, None, None), P()),
        check_vma=False,
    )
```

```python
import jax
import jax.numpy as jnp
from jax import lax
from jax.experimental import pallas as pl
from jax.experimental.pallas import tpu as pltpu
from jax.sharding import Mesh
from jax.sharding import PartitionSpec as P

GRP_MEM = ("grp_0", "grp_1", "grp_2", "mem")
GRP = ("grp_0", "grp_1", "grp_2")
TILE = 256
HALF = 128
ROWS = 6
BAND = 5
SLOTS = 11
EXTRA = 16
PREFETCH = 600
MIB = 2**20

NEAR = ((1, 5), (2, 5), (3, 4), (3, 5), (4, 5), (3, 3), (4, 4), (5, 5))
FAR = ((1, 2), (1, 3), (1, 4), (2, 3), (2, 4), (1, 1), (2, 2))


def full_of(pairs):
    return [pair for pair in pairs if pair[0] != pair[1]]


def diag_of(pairs):
    return [pair for pair in pairs if pair[0] == pair[1]]


def chunk_rows(pairs):
    return TILE * len(full_of(pairs)) + HALF * len(diag_of(pairs)) + EXTRA


def shift(value, steps):
    count = lax.axis_size(GRP_MEM)
    first, last = max(0, -steps), min(count, count - steps)
    return lax.ppermute(value, GRP_MEM, [(source, source + steps) for source in range(first, last)])


def iotas(shape):
    return lax.broadcasted_iota(jnp.int32, shape, 0), lax.broadcasted_iota(jnp.int32, shape, 1)


def smem():
    return pl.BlockSpec(memory_space=pltpu.SMEM)


def vmem():
    return pl.BlockSpec(memory_space=pltpu.VMEM)


def hbm():
    return pl.BlockSpec(memory_space=pltpu.HBM)


def params(mib):
    return pltpu.CompilerParams(vmem_limit_bytes=mib * MIB)


def cost(products, tiles_moved):
    return pl.CostEstimate(
        flops=2 * TILE**3 * products, bytes_accessed=tiles_moved * TILE * TILE * 2, transcendentals=0
    )


def write_chunk(out, pairs, first_row, branch_ref, diag_tile):
    rows, columns = iotas((HALF, HALF))
    extra_rows, _ = iotas((EXTRA, TILE))
    base = TILE * len(full_of(pairs))
    extra = jnp.zeros((EXTRA, TILE), jnp.float32)
    for place, (p, _) in enumerate(diag_of(pairs)):
        tile = diag_tile(p - 1 + first_row)
        low = tile[HALF:, HALF:]
        folded = jnp.where(columns <= rows, tile[:HALF, :HALF], low)
        at = pl.ds(base + place * HALF, HALF)
        out[at, pl.ds(0, HALF)] = tile[HALF:, :HALF].astype(jnp.bfloat16)
        out[at, pl.ds(HALF, HALF)] = folded.astype(jnp.bfloat16)
        line = jnp.sum(jnp.where(columns == rows, low, 0.0), axis=0, keepdims=True)
        line = jnp.concatenate([line, line], axis=1)
        extra = jnp.where(extra_rows == place, line, extra)
    for p in range(1, BAND + 1):
        flag = jnp.where(branch_ref[p - 1 + first_row] == 0, 0.0, 1.0)
        extra = jnp.where(extra_rows == 7 + p, flag, extra)
    out[pl.ds(base + HALF * len(diag_of(pairs)), EXTRA), :] = extra.astype(jnp.bfloat16)


def chunk_shapes(plan):
    return [jax.ShapeDtypeStruct((chunk_rows(pairs), TILE), jnp.bfloat16) for pairs, _ in plan]


def local_copies(pairs_of_refs, sems):
    copies = [
        pltpu.make_async_copy(source, target, sems.at[number])
        for number, (source, target) in enumerate(pairs_of_refs)
    ]
    for copy in copies:
        copy.start()
    return copies


def pack_corners(tiles, mask, branch, plan):
    diags = [(side, p) for side, (pairs, _) in enumerate(plan) for p, _ in diag_of(pairs)]
    fulls = [
        (side, place, p, q)
        for side, (pairs, _) in enumerate(plan)
        for place, (p, q) in enumerate(full_of(pairs))
    ]

    def body(mask_hbm, branch_hbm, tiles_ref, *refs):
        outs, refs = refs[: len(plan)], refs[len(plan) :]
        mask_ref, branch_ref, diag_ref, table_sems, full_sems, diag_sems = refs

        def spot(side, p, q):
            return p - 1 + plan[side][1], q - p + BAND

        tables = local_copies([(mask_hbm, mask_ref), (branch_hbm, branch_ref)], table_sems)
        diag_copies = local_copies(
            [(tiles_ref.at[spot(side, p, p)], diag_ref.at[number]) for number, (side, p) in enumerate(diags)],
            diag_sems,
        )
        full_copies = local_copies(
            [
                (tiles_ref.at[spot(side, p, q)], outs[side].at[pl.ds(place * TILE, TILE)])
                for side, place, p, q in fulls
            ],
            full_sems,
        )
        for copy in tables + diag_copies:
            copy.wait()
        for side, (pairs, first_row) in enumerate(plan):

            def diag_tile(row, side=side, first_row=first_row):
                number = diags.index((side, row + 1 - first_row))
                return diag_ref[number].astype(jnp.float32) * mask_ref[row, BAND].astype(jnp.float32)

            write_chunk(outs[side], pairs, first_row, branch_ref, diag_tile)
        for copy, (side, place, p, q) in zip(full_copies, fulls):
            copy.wait()

            @pl.when(mask_ref[spot(side, p, q)] == 0)
            def _(out=outs[side], place=place):
                out[pl.ds(place * TILE, TILE), :] = jnp.zeros((TILE, TILE), jnp.bfloat16)

    return pl.pallas_call(
        body,
        out_shape=chunk_shapes(plan),
        in_specs=[hbm(), hbm(), hbm()],
        out_specs=[vmem() for _ in plan],
        scratch_shapes=[
            pltpu.SMEM(mask.shape, mask.dtype),
            pltpu.SMEM(branch.shape, branch.dtype),
            pltpu.VMEM((len(diags), TILE, TILE), jnp.bfloat16),
            pltpu.SemaphoreType.DMA((2,)),
            pltpu.SemaphoreType.DMA((len(fulls),)),
            pltpu.SemaphoreType.DMA((len(diags),)),
        ],
        compiler_params=params(16),
        cost_estimate=cost(PREFETCH, PREFETCH),
        name="pack",
    )(mask, branch, tiles)


def half_scalar(value):
    return value.astype(jnp.float32).astype(jnp.bfloat16)


class Corner:
    def __init__(self, square_ref):
        self.square_ref = square_ref
        self.where = {}
        self.count = 0

    def add(self, chunk, pairs):
        rows, columns = iotas((HALF, HALF))
        for place, pair in enumerate(full_of(pairs)):
            self.where[pair] = (chunk, pl.ds(place * TILE, TILE))
        base = TILE * len(full_of(pairs))
        extra = chunk[pl.ds(base + HALF * len(diag_of(pairs)), EXTRA), :].astype(jnp.float32)
        for place, pair in enumerate(diag_of(pairs)):
            at = pl.ds(base + place * HALF, HALF)
            corner = chunk[at, pl.ds(0, HALF)].astype(jnp.float32)
            folded = chunk[at, pl.ds(HALF, HALF)].astype(jnp.float32)
            turned = folded.T
            line = extra[place : place + 1, :HALF]
            high = jnp.where(columns <= rows, folded, turned)
            low = jnp.where(columns > rows, folded, turned)
            low = jnp.where(columns == rows, line, low)
            target = self.square_ref.at[self.count]
            target[pl.ds(0, HALF), pl.ds(0, HALF)] = high.astype(jnp.bfloat16)
            target[pl.ds(HALF, HALF), pl.ds(HALF, HALF)] = low.astype(jnp.bfloat16)
            target[pl.ds(HALF, HALF), pl.ds(0, HALF)] = corner.astype(jnp.bfloat16)
            target[pl.ds(0, HALF), pl.ds(HALF, HALF)] = corner.T.astype(jnp.bfloat16)
            self.where[pair] = (target, slice(None))
            self.count += 1
        return extra

    def times(self, left, p, q):
        chunk, at = self.where[(min(p, q), max(p, q))]
        return dot(left, chunk[at, :], p > q)


def dot(left, right, transposed):
    return lax.dot_general(
        left, right, (((1,), (1 if transposed else 0,)), ((), ())), preferred_element_type=jnp.float32
    )


def polynomial(square, own, keep, bent):
    return (keep * (1.0 - 2.0 * bent)) * square + (keep * (2.0 * bent)) * own


def squares(value):
    return jnp.sum((value * value).reshape(TILE // 8, 8, TILE), axis=0)


def scalars(mask_ref, branch_ref, row, slot):
    keep = mask_ref[row, slot].astype(jnp.float32)
    bent = jnp.where(branch_ref[row] == 0, 0.0, 1.0)
    return keep, bent


def cross_outputs(up_pairs, down_pairs):
    outputs = []
    for r, q in up_pairs:
        i, j = r - 1, q - 6
        near = [((i, k - i + BAND), (k, j - k + BAND)) for k in range(q)]
        far = [((i, p - 6 - i + BAND), (p, q)) for p in range(r, BAND + 1)]
        outputs.append((i, j - i + BAND, near, far, ("above", q)))
    for r, q in down_pairs:
        i, j = q, 5 + r
        near = [((i, k - i + BAND), (k, j - k + BAND)) for k in range(r, ROWS)]
        far = [((i, 5 + p - i + BAND), (p, r)) for p in range(1, q + 1)]
        outputs.append((i, j - i + BAND, near, far, ("below", r)))
    return outputs


def near_part(tiles_ref, mask_ref, near):
    square = None
    for left, right in near:
        scale = half_scalar(mask_ref[left] * mask_ref[right])
        term = dot(tiles_ref[left] * scale, tiles_ref[right], False)
        square = term if square is None else square + term
    return square


def inner_tiles(tiles, mask, branch, outputs, plan):
    inner = [(i, j) for i in range(ROWS) for j in range(ROWS)]

    def body(mask_ref, branch_ref, tiles_ref, out_ref, sums_ref, parts_ref, *refs):
        chunks, (new_ref, out_sems) = refs[: len(plan)], refs[len(plan) :]
        rows, columns = iotas((TILE, TILE))
        total = jnp.zeros((8, TILE), jnp.float32)
        trace = jnp.zeros((8, TILE), jnp.float32)
        stores = []
        pending = []

        def emit(i, j, square):
            slot = j - i + BAND
            keep, bent = scalars(mask_ref, branch_ref, i, slot)
            value = polynomial(square, tiles_ref[i, slot].astype(jnp.float32), keep, bent)
            number = i * ROWS + j
            new_ref[number] = value
            pending.append(
                pltpu.make_async_copy(new_ref.at[number], out_ref.at[i, slot], out_sems.at[number])
            )
            return value

        def send():
            for copy in pending:
                copy.start()
            stores.extend(pending)
            pending.clear()

        def finish(i, j, square, total, trace):
            value = emit(i, j, square)
            total = total + squares(value)
            if i == j:
                part = jnp.where(rows == columns, value, 0.0)
                trace = trace + jnp.sum(part.reshape(TILE // 8, 8, TILE), axis=0)
            else:
                total = total + squares(emit(j, i, square.T))
            return total, trace

        waiting = None
        for i, j in [(i, j) for i in range(ROWS) for j in range(i, ROWS)]:
            square = None
            for k in range(j - BAND, i + BAND + 1):
                left, down = (i, k - i + BAND), 0 <= k < ROWS
                right = (k, j - k + BAND) if down else (j, k - j + BAND)
                scale = half_scalar(mask_ref[left] * mask_ref[right])
                term = dot(tiles_ref[left] * scale, tiles_ref[right], not down)
                square = term if square is None else square + term
            if waiting is not None:
                total, trace = finish(*waiting, total, trace)
            if len(pending) > GROUP:
                send()
            waiting = (i, j, square)
        total, trace = finish(*waiting, total, trace)
        send()
        sums_ref[pl.ds(0, 8), :] = total
        sums_ref[pl.ds(8, 8), :] = trace
        for number, (_, _, near, _, _) in enumerate(outputs):
            parts_ref[number] = near_part(tiles_ref, mask_ref, near)
        for (pairs, first_row), out in zip(plan, chunks):
            for place, (p, q) in enumerate(full_of(pairs)):
                spot = p - 1 + first_row, q - p + BAND
                out[pl.ds(place * TILE, TILE), :] = tiles_ref[spot] * half_scalar(mask_ref[spot])

            def diag_tile(row):
                return tiles_ref[row, BAND].astype(jnp.float32) * mask_ref[row, BAND].astype(jnp.float32)

            write_chunk(out, pairs, first_row, branch_ref, diag_tile)
        for store in stores:
            store.wait()

    products = 196 + sum(len(output[2]) for output in outputs)
    return pl.pallas_call(
        body,
        out_shape=[
            jax.ShapeDtypeStruct((ROWS, SLOTS, TILE, TILE), jnp.float32),
            jax.ShapeDtypeStruct((16, TILE), jnp.float32),
            jax.ShapeDtypeStruct((len(outputs), TILE, TILE), jnp.float32),
        ]
        + chunk_shapes(plan),
        in_specs=[smem(), smem(), vmem()],
        out_specs=[hbm()] + [vmem() for _ in range(2 + len(plan))],
        scratch_shapes=[
            pltpu.VMEM((len(inner), TILE, TILE), jnp.float32),
            pltpu.SemaphoreType.DMA((len(inner),)),
        ],
        compiler_params=params(24),
        cost_estimate=cost(products, 66 + 72),
        name="inner",
    )(mask, branch, tiles)


def table_shapes(mask, branch):
    return [
        pltpu.SMEM(mask.shape, mask.dtype),
        pltpu.SMEM(branch.shape, branch.dtype),
        pltpu.SemaphoreType.DMA((2,)),
    ]


def cross_first(tiles, mask, branch, above, below, outputs, parts, sums):
    group = 1
    for axis in GRP:
        group *= lax.axis_size(axis)

    def body(
        mask_hbm, branch_hbm, tiles_ref, above_ref, below_ref, parts_ref, sums_ref,
        new_ref, red_ref, mask_ref, branch_ref, table_sems, above_square, below_square,
    ):
        tables = local_copies([(mask_hbm, mask_ref), (branch_hbm, branch_ref)], table_sems)
        corners = {"above": Corner(above_square), "below": Corner(below_square)}
        flags = {"above": corners["above"].add(above_ref, NEAR), "below": corners["below"].add(below_ref, FAR)}
        for table in tables:
            table.wait()
        total = jnp.zeros((8, TILE), jnp.float32)

        def finish(number, square, total):
            i, slot, _, _, (side, other) = outputs[number]
            square = square + parts_ref[number]
            keep, bent = scalars(mask_ref, branch_ref, i, slot)
            mine = tiles_ref[i, slot].astype(jnp.float32)
            value = polynomial(square, mine, keep, bent)
            new_ref[number] = value
            mirror = polynomial(square, mine, keep, flags[side][7 + other : 8 + other, :])
            return total + squares(value) + squares(mirror)

        waiting = None
        for number, (_, _, _, far, (side, _)) in enumerate(outputs):
            square = None
            for left, right in far:
                term = corners[side].times(tiles_ref[left] * half_scalar(mask_ref[left]), *right)
                square = term if square is None else square + term
            if waiting is not None:
                total = finish(*waiting, total)
            waiting = (number, square)
        total = finish(*waiting, total)
        purity = jnp.sum(total + sums_ref[pl.ds(0, 8), :], keepdims=True)
        trace = jnp.sum(sums_ref[pl.ds(8, 8), :], keepdims=True)
        _, lanes = iotas((group, HALF))
        red_ref[...] = jnp.where(lanes == 0, trace, jnp.where(lanes == 1, purity, 0.0))

    return pl.pallas_call(
        body,
        out_shape=[
            jax.ShapeDtypeStruct((len(outputs), TILE, TILE), jnp.float32),
            jax.ShapeDtypeStruct((group, HALF), jnp.float32),
        ],
        in_specs=[hbm(), hbm(), vmem(), vmem(), vmem(), vmem(), vmem()],
        out_specs=[vmem(), vmem()],
        scratch_shapes=table_shapes(mask, branch)
        + [
            pltpu.VMEM((len(diag_of(NEAR)), TILE, TILE), jnp.bfloat16),
            pltpu.VMEM((len(diag_of(FAR)), TILE, TILE), jnp.bfloat16),
        ],
        compiler_params=params(16),
        cost_estimate=cost(sum(len(output[3]) for output in outputs), 66 + 2 * len(outputs)),
        name="cross_first",
    )(mask, branch, tiles, above, below, parts, sums)


GROUP = 4


def cross_last(tiles, mask, branch, made, above, below, outputs, ready_outputs, ready):
    def body(mask_hbm, branch_hbm, tiles_ref, _, ready_ref, *refs):
        chunk_refs, refs = refs[:4], refs[4:]
        (
            out_ref, mask_ref, branch_ref, table_sems, above_square, below_square, new_ref, out_sems, ready_sems,
        ) = refs
        tables = local_copies([(mask_hbm, mask_ref), (branch_hbm, branch_ref)], table_sems)
        stores = local_copies(
            [
                (ready_ref.at[number], out_ref.at[i, slot])
                for number, (i, slot, *_) in enumerate(ready_outputs)
            ],
            ready_sems,
        )
        corners = {"above": Corner(above_square), "below": Corner(below_square)}
        corners["above"].add(chunk_refs[0], NEAR)
        corners["above"].add(chunk_refs[1], FAR)
        corners["below"].add(chunk_refs[2], FAR)
        corners["below"].add(chunk_refs[3], NEAR)
        for table in tables:
            table.wait()

        def finish(number, square):
            i, slot = outputs[number][:2]
            keep, bent = scalars(mask_ref, branch_ref, i, slot)
            new_ref[number] = polynomial(square, tiles_ref[i, slot].astype(jnp.float32), keep, bent)

        def send(numbers):
            for number in numbers:
                i, slot = outputs[number][:2]
                stores.append(
                    pltpu.make_async_copy(new_ref.at[number], out_ref.at[i, slot], out_sems.at[number])
                )
                stores[-1].start()

        waiting = None
        for number, (_, _, near, far, (side, _)) in enumerate(outputs):
            square = near_part(tiles_ref, mask_ref, near)
            for left, right in far:
                square = square + corners[side].times(tiles_ref[left] * half_scalar(mask_ref[left]), *right)
            if waiting is not None:
                finish(*waiting)
            if number and number % GROUP == 0:
                send(range(number - GROUP, number))
            waiting = (number, square)
        finish(*waiting)
        send(range((len(outputs) - 1) // GROUP * GROUP, len(outputs)))
        for store in stores:
            store.wait()

    products = sum(len(output[2]) + len(output[3]) for output in outputs)
    return pl.pallas_call(
        body,
        out_shape=jax.ShapeDtypeStruct(made.shape, made.dtype),
        in_specs=[hbm(), hbm(), vmem(), hbm(), vmem()] + [vmem() for _ in range(4)],
        out_specs=hbm(),
        scratch_shapes=table_shapes(mask, branch)
        + [
            pltpu.VMEM((BAND, TILE, TILE), jnp.bfloat16),
            pltpu.VMEM((BAND, TILE, TILE), jnp.bfloat16),
            pltpu.VMEM((len(outputs), TILE, TILE), jnp.float32),
            pltpu.SemaphoreType.DMA((len(outputs),)),
            pltpu.SemaphoreType.DMA((len(ready_outputs),)),
        ],
        input_output_aliases={3: 0},
        compiler_params=params(16),
        cost_estimate=cost(products, 66 + 2 * len(outputs)),
        name="cross_last",
    )(mask, branch, tiles, made, ready, *above, *below)


def add_rows(parts):
    def body(parts_ref, out_ref):
        out_ref[...] = jnp.sum(parts_ref[...], axis=0, keepdims=True)

    return pl.pallas_call(
        body,
        out_shape=jax.ShapeDtypeStruct((1, parts.shape[1]), parts.dtype),
        in_specs=[vmem()],
        out_specs=vmem(),
        compiler_params=params(4),
        cost_estimate=cost(PREFETCH, PREFETCH),
        name="add_rows",
    )(parts)


def on_device(tiles, mask, branch):
    held, mask, branch = (
        pltpu.with_memory_space_constraint(value, pltpu.HBM) for value in (tiles, mask, branch)
    )
    down_first, up_first = pack_corners(held, mask, branch, ((NEAR, 1), (FAR, 0)))
    above_first, below_first = shift(down_first, 1), shift(up_first, -1)
    outputs = cross_outputs(NEAR, FAR)
    made, sums, parts, down_last, up_last = inner_tiles(
        tiles, mask, branch, outputs, ((FAR, 1), (NEAR, 0))
    )
    above_last = shift(down_last, 1)
    below_last = shift(up_last, -1)
    ready, part = cross_first(tiles, mask, branch, above_first, below_first, outputs, parts, sums)
    part = add_rows(lax.all_to_all(part, GRP, 0, 0, tiled=True))

    def partner(bits):
        return lax.ppermute(part, "mem", [(m, m ^ bits) for m in range(lax.axis_size("mem"))])

    others = [partner(bits) for bits in (1, 2, 3)]
    part, made = lax.optimization_barrier((part, made))
    made = cross_last(
        tiles,
        mask,
        branch,
        made,
        (above_first, above_last),
        (below_first, below_last),
        cross_outputs(FAR, NEAR),
        outputs,
        ready,
    )
    traces = (part + others[0]) + (others[1] + others[2])
    order = ROWS * lax.axis_size(GRP_MEM) * TILE
    return made, traces[0, :2] / order


def solution(mesh):
    torus = Mesh(
        mesh.devices.reshape(4, 4, 2, mesh.shape["mem"]), ("grp_0", "grp_1", "grp_2", "mem")
    )
    placed = (P(GRP_MEM, None, None, None), P(GRP_MEM, None), P(GRP_MEM))

    return jax.shard_map(
        on_device,
        mesh=torus,
        in_specs=placed,
        out_specs=(P(GRP_MEM, None, None, None), P()),
        check_vma=False,
    )
```

```python
import jax
import jax.numpy as jnp
from jax import lax
from jax.experimental import pallas as pl
from jax.experimental.pallas import tpu as pltpu
from jax.sharding import Mesh
from jax.sharding import PartitionSpec as P

GRP_MEM = ("grp_0", "grp_1", "grp_2", "mem")
GRP = ("grp_0", "grp_1", "grp_2")
TILE = 256
HALF = 128
ROWS = 6
BAND = 5
SLOTS = 11
EXTRA = 16
PREFETCH = 600
MIB = 2**20

NEAR = ((1, 5), (2, 5), (3, 4), (3, 5), (4, 5), (3, 3), (4, 4), (5, 5))
FAR = ((1, 2), (1, 3), (1, 4), (2, 3), (2, 4), (1, 1), (2, 2))


def full_of(pairs):
    return [pair for pair in pairs if pair[0] != pair[1]]


def diag_of(pairs):
    return [pair for pair in pairs if pair[0] == pair[1]]


def chunk_rows(pairs):
    return TILE * len(full_of(pairs)) + HALF * len(diag_of(pairs)) + EXTRA


CHUNK = max(chunk_rows(NEAR), chunk_rows(FAR))


def swap(value, first):
    pairs = []
    for low in range(first, lax.axis_size(GRP_MEM) - 1, 2):
        pairs += [(low, low + 1), (low + 1, low)]
    return lax.ppermute(value, GRP_MEM, pairs)


def by_parity(act):
    odd = lax.axis_index("mem") % 2
    pl.when(odd == 0)(lambda: act(True))
    pl.when(odd == 1)(lambda: act(False))


def iotas(shape):
    return lax.broadcasted_iota(jnp.int32, shape, 0), lax.broadcasted_iota(jnp.int32, shape, 1)


def smem():
    return pl.BlockSpec(memory_space=pltpu.SMEM)


def vmem():
    return pl.BlockSpec(memory_space=pltpu.VMEM)


def hbm():
    return pl.BlockSpec(memory_space=pltpu.HBM)


def params(mib):
    return pltpu.CompilerParams(vmem_limit_bytes=mib * MIB)


def cost(products, tiles_moved):
    return pl.CostEstimate(
        flops=2 * TILE**3 * products, bytes_accessed=tiles_moved * TILE * TILE * 2, transcendentals=0
    )


def write_chunk(out, pairs, first_row, branch_ref, diag_tile):
    rows, columns = iotas((HALF, HALF))
    extra_rows, _ = iotas((EXTRA, TILE))
    base = TILE * len(full_of(pairs))
    extra = jnp.zeros((EXTRA, TILE), jnp.float32)
    for place, (p, _) in enumerate(diag_of(pairs)):
        tile = diag_tile(p - 1 + first_row)
        low = tile[HALF:, HALF:]
        folded = jnp.where(columns <= rows, tile[:HALF, :HALF], low)
        at = pl.ds(base + place * HALF, HALF)
        out[at, pl.ds(0, HALF)] = tile[HALF:, :HALF].astype(jnp.bfloat16)
        out[at, pl.ds(HALF, HALF)] = folded.astype(jnp.bfloat16)
        line = jnp.sum(jnp.where(columns == rows, low, 0.0), axis=0, keepdims=True)
        line = jnp.concatenate([line, line], axis=1)
        extra = jnp.where(extra_rows == place, line, extra)
    for p in range(1, BAND + 1):
        flag = jnp.where(branch_ref[p - 1 + first_row] == 0, 0.0, 1.0)
        extra = jnp.where(extra_rows == 7 + p, flag, extra)
    out[pl.ds(base + HALF * len(diag_of(pairs)), EXTRA), :] = extra.astype(jnp.bfloat16)


def chunk_shapes(plan):
    return [jax.ShapeDtypeStruct((CHUNK, TILE), jnp.bfloat16) for _ in plan]


def local_copies(pairs_of_refs, sems):
    copies = [
        pltpu.make_async_copy(source, target, sems.at[number])
        for number, (source, target) in enumerate(pairs_of_refs)
    ]
    for copy in copies:
        copy.start()
    return copies


def pack_corners(tiles, mask, branch, plan):
    diags = [(side, p) for side, (pairs, _) in enumerate(plan) for p, _ in diag_of(pairs)]
    fulls = [
        (side, place, p, q)
        for side, (pairs, _) in enumerate(plan)
        for place, (p, q) in enumerate(full_of(pairs))
    ]

    def body(mask_hbm, branch_hbm, tiles_ref, *refs):
        by_parity(lambda even: run(even, mask_hbm, branch_hbm, tiles_ref, *refs))

    def run(even, mask_hbm, branch_hbm, tiles_ref, *refs):
        outs, refs = refs[: len(plan)], refs[len(plan) :]
        outs = outs if even else outs[::-1]
        mask_ref, branch_ref, diag_ref, table_sems, full_sems, diag_sems = refs

        def spot(side, p, q):
            return p - 1 + plan[side][1], q - p + BAND

        tables = local_copies([(mask_hbm, mask_ref), (branch_hbm, branch_ref)], table_sems)
        diag_copies = local_copies(
            [(tiles_ref.at[spot(side, p, p)], diag_ref.at[number]) for number, (side, p) in enumerate(diags)],
            diag_sems,
        )
        full_copies = local_copies(
            [
                (tiles_ref.at[spot(side, p, q)], outs[side].at[pl.ds(place * TILE, TILE)])
                for side, place, p, q in fulls
            ],
            full_sems,
        )
        for copy in tables + diag_copies:
            copy.wait()
        for side, (pairs, first_row) in enumerate(plan):

            def diag_tile(row, side=side, first_row=first_row):
                number = diags.index((side, row + 1 - first_row))
                return diag_ref[number].astype(jnp.float32) * mask_ref[row, BAND].astype(jnp.float32)

            write_chunk(outs[side], pairs, first_row, branch_ref, diag_tile)
        for copy, (side, place, p, q) in zip(full_copies, fulls):
            copy.wait()

            @pl.when(mask_ref[spot(side, p, q)] == 0)
            def _(out=outs[side], place=place):
                out[pl.ds(place * TILE, TILE), :] = jnp.zeros((TILE, TILE), jnp.bfloat16)

    return pl.pallas_call(
        body,
        out_shape=chunk_shapes(plan),
        in_specs=[hbm(), hbm(), hbm()],
        out_specs=[vmem() for _ in plan],
        scratch_shapes=[
            pltpu.SMEM(mask.shape, mask.dtype),
            pltpu.SMEM(branch.shape, branch.dtype),
            pltpu.VMEM((len(diags), TILE, TILE), jnp.bfloat16),
            pltpu.SemaphoreType.DMA((2,)),
            pltpu.SemaphoreType.DMA((len(fulls),)),
            pltpu.SemaphoreType.DMA((len(diags),)),
        ],
        compiler_params=params(16),
        cost_estimate=cost(PREFETCH, PREFETCH),
        name="pack",
    )(mask, branch, tiles)


def half_scalar(value):
    return value.astype(jnp.float32).astype(jnp.bfloat16)


class Corner:
    def __init__(self, square_ref):
        self.square_ref = square_ref
        self.where = {}
        self.count = 0

    def add(self, chunk, pairs):
        rows, columns = iotas((HALF, HALF))
        for place, pair in enumerate(full_of(pairs)):
            self.where[pair] = (chunk, pl.ds(place * TILE, TILE))
        base = TILE * len(full_of(pairs))
        extra = chunk[pl.ds(base + HALF * len(diag_of(pairs)), EXTRA), :].astype(jnp.float32)
        for place, pair in enumerate(diag_of(pairs)):
            at = pl.ds(base + place * HALF, HALF)
            corner = chunk[at, pl.ds(0, HALF)].astype(jnp.float32)
            folded = chunk[at, pl.ds(HALF, HALF)].astype(jnp.float32)
            turned = folded.T
            line = extra[place : place + 1, :HALF]
            high = jnp.where(columns <= rows, folded, turned)
            low = jnp.where(columns > rows, folded, turned)
            low = jnp.where(columns == rows, line, low)
            target = self.square_ref.at[self.count]
            target[pl.ds(0, HALF), pl.ds(0, HALF)] = high.astype(jnp.bfloat16)
            target[pl.ds(HALF, HALF), pl.ds(HALF, HALF)] = low.astype(jnp.bfloat16)
            target[pl.ds(HALF, HALF), pl.ds(0, HALF)] = corner.astype(jnp.bfloat16)
            target[pl.ds(0, HALF), pl.ds(HALF, HALF)] = corner.T.astype(jnp.bfloat16)
            self.where[pair] = (target, slice(None))
            self.count += 1
        return extra

    def times(self, left, p, q):
        chunk, at = self.where[(min(p, q), max(p, q))]
        return dot(left, chunk[at, :], p > q)


def dot(left, right, transposed):
    return lax.dot_general(
        left, right, (((1,), (1 if transposed else 0,)), ((), ())), preferred_element_type=jnp.float32
    )


def polynomial(square, own, keep, bent):
    return (keep * (1.0 - 2.0 * bent)) * square + (keep * (2.0 * bent)) * own


def squares(value):
    return jnp.sum((value * value).reshape(TILE // 8, 8, TILE), axis=0)


def scalars(mask_ref, branch_ref, row, slot):
    keep = mask_ref[row, slot].astype(jnp.float32)
    bent = jnp.where(branch_ref[row] == 0, 0.0, 1.0)
    return keep, bent


def cross_outputs(up_pairs, down_pairs):
    outputs = []
    for r, q in up_pairs:
        i, j = r - 1, q - 6
        near = [((i, k - i + BAND), (k, j - k + BAND)) for k in range(q)]
        far = [((i, p - 6 - i + BAND), (p, q)) for p in range(r, BAND + 1)]
        outputs.append((i, j - i + BAND, near, far, ("above", q)))
    for r, q in down_pairs:
        i, j = q, 5 + r
        near = [((i, k - i + BAND), (k, j - k + BAND)) for k in range(r, ROWS)]
        far = [((i, 5 + p - i + BAND), (p, r)) for p in range(1, q + 1)]
        outputs.append((i, j - i + BAND, near, far, ("below", r)))
    return outputs


def near_part(tiles_ref, mask_ref, near):
    square = None
    for left, right in near:
        scale = half_scalar(mask_ref[left] * mask_ref[right])
        term = dot(tiles_ref[left] * scale, tiles_ref[right], False)
        square = term if square is None else square + term
    return square


def inner_tiles(tiles, mask, branch, outputs, plan):
    inner = [(i, j) for i in range(ROWS) for j in range(ROWS)]

    def body(mask_ref, branch_ref, tiles_ref, out_ref, sums_ref, parts_ref, *refs):
        chunks, (new_ref, out_sems) = refs[: len(plan)], refs[len(plan) :]
        rows, columns = iotas((TILE, TILE))
        total = jnp.zeros((8, TILE), jnp.float32)
        trace = jnp.zeros((8, TILE), jnp.float32)
        stores = []
        pending = []

        def emit(i, j, square):
            slot = j - i + BAND
            keep, bent = scalars(mask_ref, branch_ref, i, slot)
            value = polynomial(square, tiles_ref[i, slot].astype(jnp.float32), keep, bent)
            number = i * ROWS + j
            new_ref[number] = value
            pending.append(
                pltpu.make_async_copy(new_ref.at[number], out_ref.at[i, slot], out_sems.at[number])
            )
            return value

        def send():
            for copy in pending:
                copy.start()
            stores.extend(pending)
            pending.clear()

        def finish(i, j, square, total, trace):
            value = emit(i, j, square)
            total = total + squares(value)
            if i == j:
                part = jnp.where(rows == columns, value, 0.0)
                trace = trace + jnp.sum(part.reshape(TILE // 8, 8, TILE), axis=0)
            else:
                total = total + squares(emit(j, i, square.T))
            return total, trace

        waiting = None
        for i, j in [(i, j) for i in range(ROWS) for j in range(i, ROWS)]:
            square = None
            for k in range(j - BAND, i + BAND + 1):
                left, down = (i, k - i + BAND), 0 <= k < ROWS
                right = (k, j - k + BAND) if down else (j, k - j + BAND)
                scale = half_scalar(mask_ref[left] * mask_ref[right])
                term = dot(tiles_ref[left] * scale, tiles_ref[right], not down)
                square = term if square is None else square + term
            if waiting is not None:
                total, trace = finish(*waiting, total, trace)
            if len(pending) > GROUP:
                send()
            waiting = (i, j, square)
        total, trace = finish(*waiting, total, trace)
        send()
        sums_ref[pl.ds(0, 8), :] = total
        sums_ref[pl.ds(8, 8), :] = trace
        for number, (_, _, near, _, _) in enumerate(outputs):
            parts_ref[number] = near_part(tiles_ref, mask_ref, near)

        def diag_tile(row):
            return tiles_ref[row, BAND].astype(jnp.float32) * mask_ref[row, BAND].astype(jnp.float32)

        def pack(even):
            for (pairs, first_row), out in zip(plan, chunks if even else chunks[::-1]):
                for place, (p, q) in enumerate(full_of(pairs)):
                    spot = p - 1 + first_row, q - p + BAND
                    out[pl.ds(place * TILE, TILE), :] = tiles_ref[spot] * half_scalar(mask_ref[spot])
                write_chunk(out, pairs, first_row, branch_ref, diag_tile)

        by_parity(pack)
        for store in stores:
            store.wait()

    products = 196 + sum(len(output[2]) for output in outputs)
    return pl.pallas_call(
        body,
        out_shape=[
            jax.ShapeDtypeStruct((ROWS, SLOTS, TILE, TILE), jnp.float32),
            jax.ShapeDtypeStruct((16, TILE), jnp.float32),
            jax.ShapeDtypeStruct((len(outputs), TILE, TILE), jnp.float32),
        ]
        + chunk_shapes(plan),
        in_specs=[smem(), smem(), vmem()],
        out_specs=[hbm()] + [vmem() for _ in range(2 + len(plan))],
        scratch_shapes=[
            pltpu.VMEM((len(inner), TILE, TILE), jnp.float32),
            pltpu.SemaphoreType.DMA((len(inner),)),
        ],
        compiler_params=params(24),
        cost_estimate=cost(products, 66 + 72),
        name="inner",
    )(mask, branch, tiles)


def sort_sides(first_ref, second_ref, above_ref, below_ref):
    def copy(even):
        above_ref[...] = (second_ref if even else first_ref)[...]
        below_ref[...] = (first_ref if even else second_ref)[...]

    by_parity(copy)


def table_shapes(mask, branch):
    return [
        pltpu.SMEM(mask.shape, mask.dtype),
        pltpu.SMEM(branch.shape, branch.dtype),
        pltpu.SemaphoreType.DMA((2,)),
    ]


def cross_first(tiles, mask, branch, swaps, outputs, parts, sums):
    group = 1
    for axis in GRP:
        group *= lax.axis_size(axis)

    def body(
        mask_hbm, branch_hbm, tiles_ref, first_ref, second_ref, parts_ref, sums_ref,
        new_ref, red_ref, above_ref, below_ref, mask_ref, branch_ref, table_sems, above_square, below_square,
    ):
        tables = local_copies([(mask_hbm, mask_ref), (branch_hbm, branch_ref)], table_sems)
        sort_sides(first_ref, second_ref, above_ref, below_ref)
        corners = {"above": Corner(above_square), "below": Corner(below_square)}
        flags = {"above": corners["above"].add(above_ref, NEAR), "below": corners["below"].add(below_ref, FAR)}
        for table in tables:
            table.wait()
        total = jnp.zeros((8, TILE), jnp.float32)

        def finish(number, square, total):
            i, slot, _, _, (side, other) = outputs[number]
            square = square + parts_ref[number]
            keep, bent = scalars(mask_ref, branch_ref, i, slot)
            mine = tiles_ref[i, slot].astype(jnp.float32)
            value = polynomial(square, mine, keep, bent)
            new_ref[number] = value
            mirror = polynomial(square, mine, keep, flags[side][7 + other : 8 + other, :])
            return total + squares(value) + squares(mirror)

        waiting = None
        for number, (_, _, _, far, (side, _)) in enumerate(outputs):
            square = None
            for left, right in far:
                term = corners[side].times(tiles_ref[left] * half_scalar(mask_ref[left]), *right)
                square = term if square is None else square + term
            if waiting is not None:
                total = finish(*waiting, total)
            waiting = (number, square)
        total = finish(*waiting, total)
        purity = jnp.sum(total + sums_ref[pl.ds(0, 8), :], keepdims=True)
        trace = jnp.sum(sums_ref[pl.ds(8, 8), :], keepdims=True)
        _, lanes = iotas((group, HALF))
        red_ref[...] = jnp.where(lanes == 0, trace, jnp.where(lanes == 1, purity, 0.0))

    return pl.pallas_call(
        body,
        out_shape=[
            jax.ShapeDtypeStruct((len(outputs), TILE, TILE), jnp.float32),
            jax.ShapeDtypeStruct((group, HALF), jnp.float32),
            jax.ShapeDtypeStruct((CHUNK, TILE), jnp.bfloat16),
            jax.ShapeDtypeStruct((CHUNK, TILE), jnp.bfloat16),
        ],
        in_specs=[hbm(), hbm(), vmem(), vmem(), vmem(), vmem(), vmem()],
        out_specs=[vmem() for _ in range(4)],
        scratch_shapes=table_shapes(mask, branch)
        + [
            pltpu.VMEM((len(diag_of(NEAR)), TILE, TILE), jnp.bfloat16),
            pltpu.VMEM((len(diag_of(FAR)), TILE, TILE), jnp.bfloat16),
        ],
        compiler_params=params(16),
        cost_estimate=cost(sum(len(output[3]) for output in outputs), 66 + 2 * len(outputs)),
        name="cross_first",
    )(mask, branch, tiles, *swaps, parts, sums)


GROUP = 4


def cross_last(tiles, mask, branch, made, sides, swaps, outputs, ready_outputs, ready):
    def body(mask_hbm, branch_hbm, tiles_ref, _, ready_ref, *refs):
        chunk_refs, refs = refs[:4], refs[4:]
        (
            out_ref, mask_ref, branch_ref, table_sems, above_ref, below_ref, above_square, below_square, new_ref,
            out_sems, ready_sems,
        ) = refs
        tables = local_copies([(mask_hbm, mask_ref), (branch_hbm, branch_ref)], table_sems)
        stores = local_copies(
            [
                (ready_ref.at[number], out_ref.at[i, slot])
                for number, (i, slot, *_) in enumerate(ready_outputs)
            ],
            ready_sems,
        )
        corners = {"above": Corner(above_square), "below": Corner(below_square)}
        sort_sides(chunk_refs[2], chunk_refs[3], above_ref, below_ref)
        corners["above"].add(chunk_refs[0], NEAR)
        corners["above"].add(above_ref, FAR)
        corners["below"].add(chunk_refs[1], FAR)
        corners["below"].add(below_ref, NEAR)
        for table in tables:
            table.wait()

        def finish(number, square):
            i, slot = outputs[number][:2]
            keep, bent = scalars(mask_ref, branch_ref, i, slot)
            new_ref[number] = polynomial(square, tiles_ref[i, slot].astype(jnp.float32), keep, bent)

        def send(numbers):
            for number in numbers:
                i, slot = outputs[number][:2]
                stores.append(
                    pltpu.make_async_copy(new_ref.at[number], out_ref.at[i, slot], out_sems.at[number])
                )
                stores[-1].start()

        waiting = None
        for number, (_, _, near, far, (side, _)) in enumerate(outputs):
            square = near_part(tiles_ref, mask_ref, near)
            for left, right in far:
                square = square + corners[side].times(tiles_ref[left] * half_scalar(mask_ref[left]), *right)
            if waiting is not None:
                finish(*waiting)
            if number and number % GROUP == 0:
                send(range(number - GROUP, number))
            waiting = (number, square)
        finish(*waiting)
        send(range((len(outputs) - 1) // GROUP * GROUP, len(outputs)))
        for store in stores:
            store.wait()

    products = sum(len(output[2]) + len(output[3]) for output in outputs)
    return pl.pallas_call(
        body,
        out_shape=jax.ShapeDtypeStruct(made.shape, made.dtype),
        in_specs=[hbm(), hbm(), vmem(), hbm(), vmem()] + [vmem() for _ in range(4)],
        out_specs=hbm(),
        scratch_shapes=table_shapes(mask, branch)
        + [
            pltpu.VMEM((CHUNK, TILE), jnp.bfloat16),
            pltpu.VMEM((CHUNK, TILE), jnp.bfloat16),
            pltpu.VMEM((BAND, TILE, TILE), jnp.bfloat16),
            pltpu.VMEM((BAND, TILE, TILE), jnp.bfloat16),
            pltpu.VMEM((len(outputs), TILE, TILE), jnp.float32),
            pltpu.SemaphoreType.DMA((len(outputs),)),
            pltpu.SemaphoreType.DMA((len(ready_outputs),)),
        ],
        input_output_aliases={3: 0},
        compiler_params=params(16),
        cost_estimate=cost(products, 66 + 2 * len(outputs)),
        name="cross_last",
    )(mask, branch, tiles, made, ready, *sides, *swaps)


def add_rows(parts):
    def body(parts_ref, out_ref):
        out_ref[...] = jnp.sum(parts_ref[...], axis=0, keepdims=True)

    return pl.pallas_call(
        body,
        out_shape=jax.ShapeDtypeStruct((1, parts.shape[1]), parts.dtype),
        in_specs=[vmem()],
        out_specs=vmem(),
        compiler_params=params(4),
        cost_estimate=cost(PREFETCH, PREFETCH),
        name="add_rows",
    )(parts)


def on_device(tiles, mask, branch):
    held, mask, branch = (
        pltpu.with_memory_space_constraint(value, pltpu.HBM) for value in (tiles, mask, branch)
    )
    packed = pack_corners(held, mask, branch, ((NEAR, 1), (FAR, 0)))
    swaps_first = [swap(packed[0], 0)]
    swaps_first.append(swap(packed[1], 1))
    outputs = cross_outputs(NEAR, FAR)
    made, sums, parts, *packed = inner_tiles(
        tiles, mask, branch, outputs, ((FAR, 1), (NEAR, 0))
    )
    swaps_last = [swap(packed[0], 0)]
    swaps_last.append(swap(packed[1], 1))
    ready, part, *sides = cross_first(tiles, mask, branch, swaps_first, outputs, parts, sums)
    part = add_rows(lax.all_to_all(part, GRP, 0, 0, tiled=True))

    def partner(bits):
        return lax.ppermute(part, "mem", [(m, m ^ bits) for m in range(lax.axis_size("mem"))])

    others = [partner(bits) for bits in (1, 2, 3)]
    part, made = lax.optimization_barrier((part, made))
    made = cross_last(
        tiles,
        mask,
        branch,
        made,
        sides,
        swaps_last,
        cross_outputs(FAR, NEAR),
        outputs,
        ready,
    )
    traces = (part + others[0]) + (others[1] + others[2])
    order = ROWS * lax.axis_size(GRP_MEM) * TILE
    return made, traces[0, :2] / order


def solution(mesh):
    torus = Mesh(
        mesh.devices.reshape(4, 4, 2, mesh.shape["mem"]), ("grp_0", "grp_1", "grp_2", "mem")
    )
    placed = (P(GRP_MEM, None, None, None), P(GRP_MEM, None), P(GRP_MEM))

    return jax.shard_map(
        on_device,
        mesh=torus,
        in_specs=placed,
        out_specs=(P(GRP_MEM, None, None, None), P()),
        check_vma=False,
    )
```
